128 devices in a mesh: tm: 8 (over z, core), rows: 16 (over x, y).
Axes of the slice: x: 4, y: 4, z: 4, core: 2. Of those that a mesh axis runs over, the one named last changes fastest.
Arguments:
- feat_mid: bfloat16 [32, 128, 128, 256], P('tm', 'rows'), may hold values from -15 to 15
- gain_mid: float32 [256], replicated, may hold values from 0.1 to 1.9
- conv_mid: bfloat16 [3, 3, 3, 256, 256], replicated, may hold values from -0.078125 to 0.078125
- down_weight: bfloat16 [8, 256, 512], replicated, may hold values from -0.125 to 0.125
- wavelets: bfloat16 [16, 24, 64, 64], P('tm', None, 'rows'), may hold values from -6 to 6
- inject_weight: bfloat16 [24, 512], replicated, may hold values from -1.25 to 1.25
- gain_deep: float32 [512], replicated, may hold values from 0.1 to 1.9
- conv_deep: bfloat16 [3, 3, 3, 512, 512], replicated, may hold values from -0.0546875 to 0.0546875
Outputs:
- encoded: bfloat16 [16, 64, 64, 512], P('tm', 'rows')
The draws below stay inside these ranges and needn't reach their ends.
All inputs are finite; a program needn't handle non-finite values.
Results may differ from the reference program's by a relative error of at most 0.0095.
Values may be sent and summed in bfloat16 or wider, within the bound.
A program may use at most 256 MiB of HBM per device.

```python
import math
import jax
import jax.numpy as jnp
from jax import lax

CH_MID = 256
CH_DEEP = 512
COLUMNS = 128
BANDS = 24
FRAMES = 32
IMG_ROWS = 128


def draw_feat_mid(key, part):
    channel_key = jax.random.fold_in(key, 11)
    value_key = jax.random.fold_in(key, 23)
    scales = jnp.exp(jax.random.uniform(channel_key, (CH_MID,), jnp.float32, math.log(0.3), math.log(3.0)))
    shape = (FRAMES, IMG_ROWS, COLUMNS, CH_MID)
    values = jnp.clip(jax.random.normal(value_key, shape, jnp.float32), -5.0, 5.0) * scales
    return values.astype(jnp.bfloat16)


def block_levels(rng, dims, pieces, least, top_value):
    level, own = 1.0, jax.random.fold_in(rng, 6)
    for dim, parts in pieces:
        draws = jnp.exp(jax.random.uniform(jax.random.fold_in(own, dim), (parts,), jnp.float32, least / len(pieces), top_value / len(pieces)))
        level = level * jnp.repeat(draws, dims[dim] // parts).reshape([-1 if axis == dim else 1 for axis in range(len(dims))])
    return level


def bell_draw(own_key, dims, width, limit, cuts=(), kind=jnp.bfloat16):
    values = jax.random.normal(own_key, dims, jnp.float32) * width
    if len(cuts) > 0:
        values = block_levels(own_key, dims, cuts, -0.22, 0.18) * values
    return jnp.clip(values, min=-limit, max=limit).astype(kind)


def setup_inputs(seed: int = 0) -> dict:
    arg_keys = jax.random.split(jax.random.key(seed), 9)
    feat_mid = draw_feat_mid(jax.random.fold_in(arg_keys[8], 71), 0)
    gain_mid = jnp.clip(1.0 + 0.18 * jax.random.normal(arg_keys[1], (CH_MID,), jnp.float32), 0.1, 1.9)
    conv_mid = bell_draw(arg_keys[2], (3, 3, 3, CH_MID, CH_MID), (27 * CH_MID) ** -0.5, 0.078125)
    down_weight = bell_draw(arg_keys[3], (8, CH_MID, CH_DEEP), (8 * CH_MID) ** -0.5, 0.125)
    wavelets = bell_draw(arg_keys[4], (FRAMES // 2, BANDS, IMG_ROWS // 2, COLUMNS // 2), 1.0, 6.0, ((0, 8), (2, 16)))
    inject_weight = bell_draw(arg_keys[5], (BANDS, CH_DEEP), BANDS ** -0.5, 1.25)
    gain_deep = jnp.clip(1.0 + 0.18 * jax.random.normal(arg_keys[6], (CH_DEEP,), jnp.float32), 0.1, 1.9)
    conv_deep = bell_draw(arg_keys[7], (3, 3, 3, CH_DEEP, CH_DEEP), (27 * CH_DEEP) ** -0.5, 0.0546875)
    return {"feat_mid": feat_mid, "gain_mid": gain_mid, "conv_mid": conv_mid, "down_weight": down_weight, "wavelets": wavelets, "inject_weight": inject_weight, "gain_deep": gain_deep, "conv_deep": conv_deep}


epsilon = 1e-06
haar_scale = 0.35355339059327373

def norm_act(values, scales):
    average = lax.optimization_barrier(jnp.mean(values, axis=-1, keepdims=True))
    centred = values - average
    spread = lax.optimization_barrier(jnp.mean(centred * centred, axis=-1, keepdims=True))
    return jax.nn.silu(centred * lax.rsqrt(spread + epsilon) * scales).astype(jnp.bfloat16)

def causal_conv(normed, weight):
    frames, height, breadth, channels = normed.shape
    padded = jnp.pad(normed, ((2, 0), (1, 1), (1, 1), (0, 0)))

    def one_frame(frame_index):
        window = lax.dynamic_slice_in_dim(padded, frame_index, 3, 0)
        summed = jnp.zeros((height * breadth, weight.shape[-1]), jnp.float32)
        for depth_tap in range(3):
            for row_tap in range(3):
                for col_tap in range(3):
                    flattened = window[depth_tap, row_tap:row_tap + height, col_tap:col_tap + breadth].reshape(height * breadth, channels)
                    summed = summed + jnp.dot(flattened, weight[depth_tap, row_tap, col_tap], preferred_element_type=jnp.float32)
        return summed.reshape(height, breadth, -1)
    return lax.map(one_frame, jnp.arange(frames, dtype=jnp.int32))

def butterfly(blocks, which_axis):
    leading = lax.index_in_dim(blocks, 0, which_axis, keepdims=False)
    trailing = lax.index_in_dim(blocks, 1, which_axis, keepdims=False)
    return (leading + trailing, leading - trailing)

def haar_project(level_two, down_weight):
    frames, height, breadth, channels = level_two.shape
    blocks = level_two.astype(jnp.float32).reshape(frames // 2, 2, height // 2, 2, breadth // 2, 2, channels)
    projected = jnp.zeros((frames // 2 * (height // 2) * (breadth // 2), down_weight.shape[-1]), jnp.float32)
    band_index = 0
    for time_part in butterfly(blocks, 1):
        for row_part in butterfly(time_part, 2):
            for col_part in butterfly(row_part, 3):
                subband = (col_part * haar_scale).astype(jnp.bfloat16).reshape(-1, channels)
                projected = projected + jnp.dot(subband, down_weight[band_index], preferred_element_type=jnp.float32)
                band_index = band_index + 1
    return projected.reshape(frames // 2, height // 2, breadth // 2, -1)

def reference(feat_mid, gain_mid, conv_mid, down_weight, wavelets, inject_weight, gain_deep, conv_deep):
    normed_mid = norm_act(feat_mid.astype(jnp.float32), gain_mid)
    conv_mid_out = causal_conv(normed_mid, conv_mid)
    level_two = (feat_mid.astype(jnp.float32) + conv_mid_out).astype(jnp.bfloat16)
    frames, height, breadth, channels = level_two.shape
    frame_pairs = level_two.reshape(frames // 2, 2, height, breadth, channels)

    def deep_frame(operands):
        frame_pair, coefficients = operands
        injected = jnp.einsum('bhw,bd->hwd', coefficients.astype(jnp.float32), inject_weight.astype(jnp.float32), precision=lax.Precision.HIGHEST)
        return haar_project(frame_pair, down_weight)[0] + injected
    feat_deep = lax.map(deep_frame, (frame_pairs, wavelets))
    normed_deep = norm_act(feat_deep, gain_deep)
    conv_deep_out = causal_conv(normed_deep, conv_deep)
    return (feat_deep + conv_deep_out).astype(jnp.bfloat16)
```

```python
import functools

import jax
import jax.numpy as jnp
from jax import lax
from jax.experimental import pallas as pl
from jax.experimental.pallas import tpu as pltpu
from jax.sharding import PartitionSpec as P

epsilon = 1e-06
haar_scale = 0.35355339059327373
MESH = pl.DeviceIdType.MESH
BF = jnp.bfloat16
F32 = jnp.float32


def norm_silu(x, half_gain):
    mean = jnp.mean(x, axis=-1, keepdims=True)
    c = x - mean
    var = jnp.mean(c * c, axis=-1, keepdims=True)
    h = c * lax.rsqrt(var + epsilon) * half_gain
    return (h + h * jnp.tanh(h)).astype(BF)


def shift_down(x):
    row = lax.broadcasted_iota(jnp.int32, x.shape, 0)
    return jnp.where(row == 0, 0.0, pltpu.roll(x, 1, 0))


def shift_up(x):
    n = x.shape[0]
    row = lax.broadcasted_iota(jnp.int32, x.shape, 0)
    return jnp.where(row == n - 1, 0.0, pltpu.roll(x, n - 1, 0))


def kernel(
    n_tm, n_rows,
    feat, gain_mid, conv_mid, down, wav, inj, gain_deep, conv_deep,
    out,
    fv, wm, wdn, wd, wv, iv, injw, wavt, xp, ym, lv, sb, fd, yp, yd, ov,
    lsem, send, recv, osem,
    *accs,
):
    t_id, r_id = lax.axis_index("tm"), lax.axis_index("rows")
    has_prev, has_next = t_id > 0, t_id < n_tm - 1
    has_up, has_dn = r_id > 0, r_id < n_rows - 1
    acc = (accs[:6], accs[6:])

    def load(i, src, dst):
        return pltpu.make_async_copy(src, dst, lsem.at[i])

    feat_loads = [load(i, feat.at[i], fv.at[i]) for i in range(4)]
    for i in (3, 2, 1, 0):
        feat_loads[i].start()
    ld_wm = load(4, conv_mid, wm)
    ld_dn = load(5, down, wdn)
    ld_wv = load(6, wav, wv)
    ld_iv = load(7, inj, iv)
    ld_wd = load(8, conv_deep, wd)
    for ld in (ld_wm, ld_wv, ld_iv, ld_dn, ld_wd):
        ld.start()

    barrier = pltpu.get_barrier_semaphore()
    count = jnp.int32(0)
    for dt in (-1, 0, 1):
        for dr in (-1, 0, 1):
            if dt == 0 and dr == 0:
                continue
            there = jnp.bool_(True)
            if dt:
                there = has_prev if dt < 0 else has_next
            if dr:
                there_r = has_up if dr < 0 else has_dn
                there = jnp.logical_and(there, there_r) if dt else there_r
            count = count + there.astype(jnp.int32)

            @pl.when(there)
            def _():
                pl.semaphore_signal(
                    barrier, inc=1, device_id=(t_id + dt, r_id + dr), device_id_type=MESH
                )

    halo = {}

    def both(dt, dr):
        cond = {-1: (has_prev, has_up), 1: (has_next, has_dn)}
        target, source = None, None
        if dt:
            target, source = cond[dt][0], cond[-dt][0]
        if dr:
            tr, sr = cond[dr][1], cond[-dr][1]
            target = tr if target is None else jnp.logical_and(target, tr)
            source = sr if source is None else jnp.logical_and(source, sr)
        return target, source

    def add_halo(name, src, dst, dt, dr):
        i = len(halo)
        desc = pltpu.make_async_remote_copy(
            src_ref=src, dst_ref=dst, send_sem=send.at[i], recv_sem=recv.at[i],
            device_id=(t_id + dt, r_id + dr), device_id_type=MESH,
        )
        target, source = both(dt, dr)
        halo[name] = (desc, target, source)

    add_halo("u23", xp.at[4:6, 1], xp.at[4:6, 9], 0, -1)
    add_halo("d23", xp.at[4:6, 8], xp.at[4:6, 0], 0, 1)
    add_halo("u01", xp.at[2:4, 1], xp.at[2:4, 9], 0, -1)
    add_halo("d01", xp.at[2:4, 8], xp.at[2:4, 0], 0, 1)
    add_halo("z3", xp.at[5, 1:9], xp.at[1, 1:9], 1, 0)
    add_halo("z2", xp.at[4, 1:9], xp.at[0, 1:9], 1, 0)
    add_halo("zu", xp.at[4:6, 1], xp.at[0:2, 9], 1, -1)
    add_halo("zd", xp.at[4:6, 8], xp.at[0:2, 0], 1, 1)
    for f in (1, 0):
        add_halo(f"yu{f}", yp.at[2 + f, 1], yp.at[2 + f, 5], 0, -1)
        add_halo(f"yd{f}", yp.at[2 + f, 4], yp.at[2 + f, 0], 0, 1)
        add_halo(f"yz{f}", yp.at[2 + f, 1:5], yp.at[f, 1:5], 1, 0)
        add_halo(f"yzu{f}", yp.at[2 + f, 1], yp.at[f, 5], 1, -1)
        add_halo(f"yzd{f}", yp.at[2 + f, 4], yp.at[f, 0], 1, 1)

    def start(*names):
        for name in names:
            desc, target, _ = halo[name]
            pl.when(target)(desc.start)

    def arrive(*names):
        for name in names:
            desc, _, source = halo[name]
            pl.when(source)(desc.wait_recv)

    @pl.when(jnp.logical_not(has_prev))
    def _():
        xp[0:2] = jnp.zeros((2, 10, 128, 256), BF)
        yp[0:2] = jnp.zeros((2, 6, 64, 512), BF)

    @pl.when(jnp.logical_not(has_up))
    def _():
        xp[:, 0] = jnp.zeros((6, 128, 256), BF)
        yp[:, 0] = jnp.zeros((4, 64, 512), BF)

    @pl.when(jnp.logical_not(has_dn))
    def _():
        xp[:, 9] = jnp.zeros((6, 128, 256), BF)
        yp[:, 5] = jnp.zeros((4, 64, 512), BF)

    half_gain = gain_mid[...] * 0.5

    def norm_frame(f):
        feat_loads[f].wait()

        @pl.loop(0, 8)
        def _(r):
            for piece in range(2):
                rows = pl.ds(piece * 64, 64)
                xp[f + 2, r + 1, rows, :] = norm_silu(fv[f, r, rows, :].astype(F32), half_gain)

    norm_frame(3)
    norm_frame(2)
    pl.semaphore_wait(barrier, count)
    start("u23", "d23", "z3", "z2", "zu", "zd")
    norm_frame(1)
    norm_frame(0)
    start("u01", "d01")

    injw[...] = jnp.zeros((256, 512), BF)
    wavt[...] = jnp.zeros((2, 256, 256), BF)
    ld_wv.wait()
    ld_iv.wait()
    injw[0:24, :] = iv[...]
    for t in range(2):
        coeffs = wv[t].astype(F32)
        for h in range(4):
            wavt[t, h * 64:(h + 1) * 64, 0:24] = coeffs[:, h, :].T.astype(BF)

    def mid_block(t, first_rows, slot):
        k = 0
        for c in range(3):
            for a in range(3):
                for b in range(3):
                    tap = (a * 3 + b) * 3 + c
                    for q in range(2):
                        pltpu.matmul_push_rhs(wm[tap], k % 2, q)
                        for h in range(2):
                            pltpu.matmul_acc_lhs(
                                acc[q][c * 2 + h], xp[t + a, first_rows[q] + b + h],
                                load_staged_rhs=k % 2 if h == 0 else None,
                            )
                    k += 1
            for q in range(2):
                for h in range(2):
                    ym[slot, q, h, c] = pltpu.matmul_pop(acc[q][c * 2 + h])

    def mid_combine(t, first_rows, slot):
        for q in range(2):
            for h in range(2):
                r = first_rows[q] + h
                for n in range(2):
                    lanes = pl.ds(n * 128, 128)
                    total = shift_down(ym[slot, q, h, 0, :, lanes]) + ym[slot, q, h, 1, :, lanes]
                    total = total + shift_up(ym[slot, q, h, 2, :, lanes])
                    level = (fv[t, r, :, lanes].astype(F32) + total).astype(BF)
                    lv[t % 2, n, r] = level.astype(F32)

    inner, outer = (2, 4), (0, 6)

    def mid_pair(t0, first_rows):
        for i in range(2):
            mid_block(t0 + i, first_rows, i)
            mid_combine(t0 + i, first_rows, i)

    half_gain_deep = gain_deep[...] * 0.5

    def deep_frame(t):
        @pl.loop(0, 4)
        def _(r):
            for piece in range(4):
                for n in range(2):
                    lanes = pl.ds(n * 128, 128)
                    v = {}
                    for i in range(2):
                        for j in range(2):
                            for k in range(2):
                                v[i, j, k] = lv[
                                    i, n, 2 * r + j, pl.ds(piece * 32 + k, 16, stride=2), :
                                ]
                    for axis in range(3):
                        w = {}
                        for key in v:
                            if key[axis] == 0:
                                other = key[:axis] + (1,) + key[axis + 1:]
                                w[key] = v[key] + v[other]
                                w[other] = v[key] - v[other]
                        v = w
                    for i in range(2):
                        for j in range(2):
                            for k in range(2):
                                s = 4 * i + 2 * j + k
                                row = pl.multiple_of(r * 64 + piece * 16, 16)
                                sb[s, pl.ds(row, 16), lanes] = (v[i, j, k] * haar_scale).astype(BF)

        for s in range(9):
            for q in range(2):
                cols = slice(q * 256, (q + 1) * 256)
                rhs = wdn[s, :, cols] if s < 8 else injw[:, cols]
                pltpu.matmul_push_rhs(rhs, s % 2, q)
                for h in range(2):
                    rows = slice(h * 128, (h + 1) * 128)
                    lhs = sb[s, rows, :] if s < 8 else wavt[t, rows, :]
                    pltpu.matmul_acc_lhs(acc[q][h], lhs, load_staged_rhs=s % 2 if h == 0 else None)
        for h in range(2):
            for q in range(2):
                fd[t, h * 128:(h + 1) * 128, q * 256:(q + 1) * 256] = pltpu.matmul_pop(acc[q][h])

        @pl.loop(0, 4)
        def _(r):
            for piece in range(2):
                rows = pl.ds(pl.multiple_of(r * 64 + piece * 32, 32), 32)
                yp[t + 2, r + 1, pl.ds(piece * 32, 32), :] = norm_silu(fd[t, rows, :], half_gain_deep)

    def start_deep(f):
        start(f"yu{f}", f"yd{f}", f"yz{f}", f"yzu{f}", f"yzd{f}")

    ld_wm.wait()
    mid_pair(2, inner)
    arrive("u23", "d23", "u01", "d01")
    mid_pair(2, outer)
    ld_dn.wait()
    deep_frame(1)
    start_deep(1)
    arrive("z3", "z2", "zu", "zd")
    mid_pair(0, inner)
    mid_pair(0, outer)
    deep_frame(0)
    start_deep(0)

    ld_wd.wait()

    def deep_conv(t, order, waits):
        k = 0
        for step, a in enumerate(order):
            arrive(*waits[step])
            for c in range(3):
                for b in range(3):
                    tap = (a * 3 + b) * 3 + c
                    for d in range(2):
                        depth = slice(d * 256, (d + 1) * 256)
                        for q in range(2):
                            pltpu.matmul_push_rhs(
                                wd[tap, depth, q * 256:(q + 1) * 256], k % 2, q
                            )
                            for h in range(2):
                                lhs = yp[t + a, b + 2 * h:b + 2 * h + 2, :, depth]
                                pltpu.matmul_acc_lhs(
                                    acc[q][c * 2 + h], lhs.reshape(128, 256),
                                    load_staged_rhs=k % 2 if h == 0 else None,
                                )
                        k += 1
                if step == 2:
                    for q in range(2):
                        for h in range(2):
                            yd[t, c, h * 128:(h + 1) * 128, q * 256:(q + 1) * 256] = (
                                pltpu.matmul_pop(acc[q][c * 2 + h])
                            )

    def deep_combine(t):
        for r in range(4):
            rows = slice(r * 64, (r + 1) * 64)
            for n in range(4):
                lanes = slice(n * 128, (n + 1) * 128)
                total = shift_down(yd[t, 0, rows, lanes]) + yd[t, 1, rows, lanes]
                total = total + shift_up(yd[t, 2, rows, lanes])
                ov[t, r, :, lanes] = (fd[t, rows, lanes] + total).astype(BF)

    deep_conv(1, (2, 0, 1), (("yu1", "yd1"), ("yz1", "yzu1", "yzd1"), ("yu0", "yd0")))
    deep_combine(1)
    store1 = pltpu.make_async_copy(ov.at[1], out.at[1], osem.at[1])
    store1.start()
    deep_conv(0, (1, 2, 0), ((), (), ("yz0", "yzu0", "yzd0")))
    deep_combine(0)
    store0 = pltpu.make_async_copy(ov.at[0], out.at[0], osem.at[0])
    store0.start()

    for desc, target, _ in halo.values():
        pl.when(target)(desc.wait_send)
    store1.wait()
    store0.wait()


def on_device(n_tm, n_rows, feat, gain_mid, conv_mid, down, wav, inj, gain_deep, conv_deep):
    def body(*refs):
        def inner(*accs):
            kernel(n_tm, n_rows, *refs, *accs)

        pl.run_scoped(inner, *[pltpu.ACC(q)((128, 256), F32) for q in range(2) for _ in range(6)])

    hbm = pl.BlockSpec(memory_space=pl.ANY)
    vmem = pl.BlockSpec(memory_space=pltpu.VMEM)
    return pl.pallas_call(
        body,
        out_shape=jax.ShapeDtypeStruct((2, 4, 64, 512), BF),
        in_specs=[hbm, vmem, hbm, hbm, hbm, hbm, vmem, hbm],
        out_specs=hbm,
        scratch_shapes=[
            pltpu.VMEM((4, 8, 128, 256), BF),
            pltpu.VMEM((27, 256, 256), BF),
            pltpu.VMEM((8, 256, 512), BF),
            pltpu.VMEM((27, 512, 512), BF),
            pltpu.VMEM((2, 24, 4, 64), BF),
            pltpu.VMEM((24, 512), BF),
            pltpu.VMEM((256, 512), BF),
            pltpu.VMEM((2, 256, 256), BF),
            pltpu.VMEM((6, 10, 128, 256), BF),
            pltpu.VMEM((2, 2, 2, 3, 128, 256), F32),
            pltpu.VMEM((2, 2, 8, 128, 128), F32),
            pltpu.VMEM((8, 256, 256), BF),
            pltpu.VMEM((2, 256, 512), F32),
            pltpu.VMEM((4, 6, 64, 512), BF),
            pltpu.VMEM((2, 3, 256, 512), F32),
            pltpu.VMEM((2, 4, 64, 512), BF),
            pltpu.SemaphoreType.DMA((9,)),
            pltpu.SemaphoreType.DMA((18,)),
            pltpu.SemaphoreType.DMA((18,)),
            pltpu.SemaphoreType.DMA((2,)),
        ],
        compiler_params=pltpu.CompilerParams(
            collective_id=0, has_side_effects=True, vmem_limit_bytes=64 * 1000 * 1000
        ),
    )(
        feat, gain_mid.reshape(1, 256), conv_mid.reshape(27, 256, 256), down, wav, inj,
        gain_deep.reshape(1, 512), conv_deep.reshape(27, 512, 512),
    )


def solution(mesh):
    return jax.shard_map(
        functools.partial(on_device, mesh.shape["tm"], mesh.shape["rows"]),
        mesh=mesh,
        in_specs=(
            P("tm", "rows", None, None), P(), P(), P(), P("tm", None, "rows", None), P(), P(), P(),
        ),
        out_specs=P("tm", "rows", None, None),
        check_vma=False,
    )
```

```python
import functools

import jax
import jax.numpy as jnp
from jax import lax
from jax.experimental import pallas as pl
from jax.experimental.pallas import tpu as pltpu
from jax.sharding import PartitionSpec as P

epsilon = 1e-06
haar_scale = 0.35355339059327373
MESH = pl.DeviceIdType.MESH
BF = jnp.bfloat16
F32 = jnp.float32


def norm_silu(x, half_gain):
    mean = jnp.mean(x, axis=-1, keepdims=True)
    c = x - mean
    var = jnp.mean(c * c, axis=-1, keepdims=True)
    h = c * lax.rsqrt(var + epsilon) * half_gain
    return (h + h * jnp.tanh(h)).astype(BF)


def shift_down(x):
    row = lax.broadcasted_iota(jnp.int32, x.shape, 0)
    return jnp.where(row == 0, 0.0, pltpu.roll(x, 1, 0))


def shift_up(x):
    n = x.shape[0]
    row = lax.broadcasted_iota(jnp.int32, x.shape, 0)
    return jnp.where(row == n - 1, 0.0, pltpu.roll(x, n - 1, 0))


def kernel(
    n_tm, n_rows,
    feat, gain_mid, conv_mid, down, wav, inj, gain_deep, conv_deep,
    out,
    fv, wm, wdn, wd, wv, iv, injw, wavt, xp, ym, ye, lv, sb, fd, yp, yd, ov,
    lsem, send, recv, osem,
    *accs,
):
    t_id, r_id = lax.axis_index("tm"), lax.axis_index("rows")
    has_prev, has_next = t_id > 0, t_id < n_tm - 1
    has_up, has_dn = r_id > 0, r_id < n_rows - 1
    acc = (accs[:6], accs[6:])

    def load(i, src, dst):
        return pltpu.make_async_copy(src, dst, lsem.at[i])

    feat_loads = [load(i, feat.at[i], fv.at[i]) for i in range(4)]
    for i in (3, 2, 1, 0):
        feat_loads[i].start()
    ld_wm = load(4, conv_mid, wm)
    ld_dn = load(5, down, wdn)
    ld_wv = load(6, wav, wv)
    ld_iv = load(7, inj, iv)
    ld_wd = load(8, conv_deep, wd)
    for ld in (ld_wm, ld_wv, ld_iv, ld_dn, ld_wd):
        ld.start()

    barrier = pltpu.get_barrier_semaphore()
    count = jnp.int32(0)
    for dt in (-1, 0, 1):
        for dr in (-1, 0, 1):
            if dt == 0 and dr == 0:
                continue
            there = jnp.bool_(True)
            if dt:
                there = has_prev if dt < 0 else has_next
            if dr:
                there_r = has_up if dr < 0 else has_dn
                there = jnp.logical_and(there, there_r) if dt else there_r
            count = count + there.astype(jnp.int32)

            @pl.when(there)
            def _():
                pl.semaphore_signal(
                    barrier, inc=1, device_id=(t_id + dt, r_id + dr), device_id_type=MESH
                )

    halo = {}

    def both(dt, dr):
        cond = {-1: (has_prev, has_up), 1: (has_next, has_dn)}
        target, source = None, None
        if dt:
            target, source = cond[dt][0], cond[-dt][0]
        if dr:
            tr, sr = cond[dr][1], cond[-dr][1]
            target = tr if target is None else jnp.logical_and(target, tr)
            source = sr if source is None else jnp.logical_and(source, sr)
        return target, source

    def add_halo(name, src, dst, dt, dr, only=None):
        i = len(halo)
        desc = pltpu.make_async_remote_copy(
            src_ref=src, dst_ref=dst, send_sem=send.at[i], recv_sem=recv.at[i],
            device_id=(t_id + dt, r_id + dr), device_id_type=MESH,
        )
        target, source = both(dt, dr)
        if only is not None:
            target, source = jnp.logical_and(target, only), jnp.logical_and(source, only)
        halo[name] = (desc, target, source)

    add_halo("u", xp.at[2:6, 1], xp.at[2:6, 9], 0, -1)
    add_halo("d", xp.at[2:6, 8], xp.at[2:6, 0], 0, 1)
    add_halo("ze1", xp.at[4:6, 1], xp.at[0:2, 1], 1, 0)
    add_halo("ze8", xp.at[4:6, 8], xp.at[0:2, 8], 1, 0)
    add_halo("z3", xp.at[5, 2:8], xp.at[1, 2:8], 1, 0)
    add_halo("z2", xp.at[4, 2:8], xp.at[0, 2:8], 1, 0)
    add_halo("cu", xp.at[0:2, 1], xp.at[0:2, 9], 0, -1, has_prev)
    add_halo("cd", xp.at[0:2, 8], xp.at[0:2, 0], 0, 1, has_prev)
    for f in (1, 0):
        add_halo(f"yu{f}", yp.at[2 + f, 1], yp.at[2 + f, 5], 0, -1)
        add_halo(f"yd{f}", yp.at[2 + f, 4], yp.at[2 + f, 0], 0, 1)
        add_halo(f"yz{f}", yp.at[2 + f, 1:5], yp.at[f, 1:5], 1, 0)
        add_halo(f"yzu{f}", yp.at[2 + f, 1], yp.at[f, 5], 1, -1)
        add_halo(f"yzd{f}", yp.at[2 + f, 4], yp.at[f, 0], 1, 1)

    def start(*names):
        for name in names:
            desc, target, _ = halo[name]
            pl.when(target)(desc.start)

    def arrive(*names):
        for name in names:
            desc, _, source = halo[name]
            pl.when(source)(desc.wait_recv)

    @pl.when(jnp.logical_not(has_prev))
    def _():
        xp[0:2] = jnp.zeros((2, 10, 128, 256), BF)
        yp[0:2] = jnp.zeros((2, 6, 64, 512), BF)

    @pl.when(jnp.logical_not(has_up))
    def _():
        xp[:, 0] = jnp.zeros((6, 128, 256), BF)
        yp[:, 0] = jnp.zeros((4, 64, 512), BF)

    @pl.when(jnp.logical_not(has_dn))
    def _():
        xp[:, 9] = jnp.zeros((6, 128, 256), BF)
        yp[:, 5] = jnp.zeros((4, 64, 512), BF)

    half_gain = gain_mid[...] * 0.5

    def norm_row(f, r):
        for piece in range(2):
            rows = pl.ds(piece * 64, 64)
            xp[f + 2, r + 1, rows, :] = norm_silu(fv[f, r, rows, :].astype(F32), half_gain)

    for f in (3, 2, 1, 0):
        feat_loads[f].wait()

    @pl.loop(0, 4)
    def _(f):
        norm_row(f, 0)
        norm_row(f, 7)

    pl.semaphore_wait(barrier, count)
    start("u", "d", "ze1", "ze8")
    for f in (3, 2, 1):
        @pl.loop(0, 3)
        def _(r):
            norm_row(f, 2 * r + 1)
            norm_row(f, 2 * r + 2)

        if f == 3:
            start("z3")
        if f == 2:
            start("z2")

    injw[...] = jnp.zeros((256, 512), BF)
    wavt[...] = jnp.zeros((2, 256, 256), BF)
    ld_wv.wait()
    ld_iv.wait()
    injw[0:24, :] = iv[...]
    for t in range(2):
        coeffs = wv[t].astype(F32)
        for h in range(4):
            wavt[t, h * 64:(h + 1) * 64, 0:24] = coeffs[:, h, :].T.astype(BF)

    bands = ((2, 4), (0, 6))

    def mid_block(t, band, depths, dst, base=None):
        k = 0
        for c in range(3):
            for a in depths:
                for b in range(3):
                    tap = (a * 3 + b) * 3 + c
                    for q in range(2):
                        pltpu.matmul_push_rhs(wm[tap], k % 2, q)
                        for h in range(2):
                            pltpu.matmul_acc_lhs(
                                acc[q][c * 2 + h], xp[t + a, bands[band][q] + b + h],
                                load_staged_rhs=k % 2 if h == 0 else None,
                            )
                    k += 1
            for q in range(2):
                for h in range(2):
                    total = pltpu.matmul_pop(acc[q][c * 2 + h])
                    if base is not None:
                        total = total + base[q, h, c]
                    dst[q, h, c] = total

    def mid_combine(t, band, src):
        for q in range(2):
            for h in range(2):
                r = bands[band][q] + h
                for n in range(2):
                    lanes = pl.ds(n * 128, 128)
                    total = shift_down(src[q, h, 0, :, lanes]) + src[q, h, 1, :, lanes]
                    total = total + shift_up(src[q, h, 2, :, lanes])
                    level = (fv[t, r, :, lanes].astype(F32) + total).astype(BF)
                    lv[t % 2, n, r] = level.astype(F32)

    def mid_full(t, band, slot):
        mid_block(t, band, (0, 1, 2), ym.at[slot])
        mid_combine(t, band, ym.at[slot])

    def mid_early(t, band):
        mid_block(t, band, (2, 1) if t == 1 else (2,), ye.at[t, band])

    def mid_late(t, band, slot):
        mid_block(t, band, (0,) if t == 1 else (1, 0), ym.at[slot], ye.at[t, band])
        mid_combine(t, band, ym.at[slot])

    half_gain_deep = gain_deep[...] * 0.5

    def deep_frame(t):
        @pl.loop(0, 4)
        def _(r):
            for piece in range(4):
                for n in range(2):
                    lanes = pl.ds(n * 128, 128)
                    v = {}
                    for i in range(2):
                        for j in range(2):
                            for k in range(2):
                                v[i, j, k] = lv[
                                    i, n, 2 * r + j, pl.ds(piece * 32 + k, 16, stride=2), :
                                ]
                    for axis in range(3):
                        w = {}
                        for key in v:
                            if key[axis] == 0:
                                other = key[:axis] + (1,) + key[axis + 1:]
                                w[key] = v[key] + v[other]
                                w[other] = v[key] - v[other]
                        v = w
                    for i in range(2):
                        for j in range(2):
                            for k in range(2):
                                s = 4 * i + 2 * j + k
                                row = pl.multiple_of(r * 64 + piece * 16, 16)
                                sb[s, pl.ds(row, 16), lanes] = (v[i, j, k] * haar_scale).astype(BF)

        for s in range(9):
            for q in range(2):
                cols = slice(q * 256, (q + 1) * 256)
                rhs = wdn[s, :, cols] if s < 8 else injw[:, cols]
                pltpu.matmul_push_rhs(rhs, s % 2, q)
                for h in range(2):
                    rows = slice(h * 128, (h + 1) * 128)
                    lhs = sb[s, rows, :] if s < 8 else wavt[t, rows, :]
                    pltpu.matmul_acc_lhs(acc[q][h], lhs, load_staged_rhs=s % 2 if h == 0 else None)
        for h in range(2):
            for q in range(2):
                fd[t, h * 128:(h + 1) * 128, q * 256:(q + 1) * 256] = pltpu.matmul_pop(acc[q][h])

        @pl.loop(0, 4)
        def _(r):
            for piece in range(2):
                rows = pl.ds(pl.multiple_of(r * 64 + piece * 32, 32), 32)
                yp[t + 2, r + 1, pl.ds(piece * 32, 32), :] = norm_silu(fd[t, rows, :], half_gain_deep)

    def start_deep(f):
        start(f"yu{f}", f"yd{f}", f"yz{f}", f"yzu{f}", f"yzd{f}")

    ld_wm.wait()
    mid_full(3, 0, 0)
    for r in range(1, 7):
        norm_row(0, r)
    mid_full(2, 0, 1)
    arrive("ze1", "ze8")
    start("cu", "cd")
    mid_early(1, 0)
    mid_early(0, 0)
    arrive("u", "d")
    mid_full(3, 1, 0)
    mid_full(2, 1, 1)
    ld_dn.wait()
    deep_frame(1)
    start_deep(1)
    mid_early(1, 1)
    mid_early(0, 1)
    arrive("z3", "cu", "cd")
    mid_late(1, 0, 0)
    mid_late(1, 1, 1)
    arrive("z2")
    mid_late(0, 0, 0)
    mid_late(0, 1, 1)
    deep_frame(0)
    start_deep(0)

    ld_wd.wait()

    def deep_conv(t, order, base=None):
        k = 0
        for step, (a, names) in enumerate(order):
            arrive(*names)
            for c in range(3):
                for b in range(3):
                    tap = (a * 3 + b) * 3 + c
                    for d in range(2):
                        depth = slice(d * 256, (d + 1) * 256)
                        for q in range(2):
                            pltpu.matmul_push_rhs(
                                wd[tap, depth, q * 256:(q + 1) * 256], k % 2, q
                            )
                            for h in range(2):
                                lhs = yp[t + a, b + 2 * h:b + 2 * h + 2, :, depth]
                                pltpu.matmul_acc_lhs(
                                    acc[q][c * 2 + h], lhs.reshape(128, 256),
                                    load_staged_rhs=k % 2 if h == 0 else None,
                                )
                        k += 1
                if step == len(order) - 1:
                    for q in range(2):
                        for h in range(2):
                            block = (c, slice(h * 128, (h + 1) * 128), slice(q * 256, (q + 1) * 256))
                            total = pltpu.matmul_pop(acc[q][c * 2 + h])
                            if base is not None:
                                total = total + base[block]
                            yd[(t,) + block] = total

    def deep_combine(t):
        for r in range(4):
            rows = slice(r * 64, (r + 1) * 64)
            for n in range(4):
                lanes = slice(n * 128, (n + 1) * 128)
                total = shift_down(yd[t, 0, rows, lanes]) + yd[t, 1, rows, lanes]
                total = total + shift_up(yd[t, 2, rows, lanes])
                ov[t, r, :, lanes] = (fd[t, rows, lanes] + total).astype(BF)

    arrive("yu1", "yd1", "yz1", "yzu1", "yzd1")
    deep_conv(0, ((1, ()),))
    deep_conv(1, ((2, ()), (0, ()), (1, ("yu0", "yd0"))))
    deep_combine(1)
    store1 = pltpu.make_async_copy(ov.at[1], out.at[1], osem.at[1])
    store1.start()
    deep_conv(0, ((2, ()), (0, ("yz0", "yzu0", "yzd0"))), yd.at[0])
    deep_combine(0)
    store0 = pltpu.make_async_copy(ov.at[0], out.at[0], osem.at[0])
    store0.start()

    for desc, target, _ in halo.values():
        pl.when(target)(desc.wait_send)
    store1.wait()
    store0.wait()


def on_device(n_tm, n_rows, feat, gain_mid, conv_mid, down, wav, inj, gain_deep, conv_deep):
    def body(*refs):
        def inner(*accs):
            kernel(n_tm, n_rows, *refs, *accs)

        pl.run_scoped(inner, *[pltpu.ACC(q)((128, 256), F32) for q in range(2) for _ in range(6)])

    hbm = pl.BlockSpec(memory_space=pl.ANY)
    vmem = pl.BlockSpec(memory_space=pltpu.VMEM)
    return pl.pallas_call(
        body,
        out_shape=jax.ShapeDtypeStruct((2, 4, 64, 512), BF),
        in_specs=[hbm, vmem, hbm, hbm, hbm, hbm, vmem, hbm],
        out_specs=hbm,
        scratch_shapes=[
            pltpu.VMEM((4, 8, 128, 256), BF),
            pltpu.VMEM((27, 256, 256), BF),
            pltpu.VMEM((8, 256, 512), BF),
            pltpu.VMEM((27, 512, 512), BF),
            pltpu.VMEM((2, 24, 4, 64), BF),
            pltpu.VMEM((24, 512), BF),
            pltpu.VMEM((256, 512), BF),
            pltpu.VMEM((2, 256, 256), BF),
            pltpu.VMEM((6, 10, 128, 256), BF),
            pltpu.VMEM((2, 2, 2, 3, 128, 256), F32),
            pltpu.VMEM((2, 2, 2, 2, 3, 128, 256), F32),
            pltpu.VMEM((2, 2, 8, 128, 128), F32),
            pltpu.VMEM((8, 256, 256), BF),
            pltpu.VMEM((2, 256, 512), F32),
            pltpu.VMEM((4, 6, 64, 512), BF),
            pltpu.VMEM((2, 3, 256, 512), F32),
            pltpu.VMEM((2, 4, 64, 512), BF),
            pltpu.SemaphoreType.DMA((9,)),
            pltpu.SemaphoreType.DMA((18,)),
            pltpu.SemaphoreType.DMA((18,)),
            pltpu.SemaphoreType.DMA((2,)),
        ],
        compiler_params=pltpu.CompilerParams(
            collective_id=0, has_side_effects=True, vmem_limit_bytes=64 * 1000 * 1000
        ),
    )(
        feat, gain_mid.reshape(1, 256), conv_mid.reshape(27, 256, 256), down, wav, inj,
        gain_deep.reshape(1, 512), conv_deep.reshape(27, 512, 512),
    )


def solution(mesh):
    return jax.shard_map(
        functools.partial(on_device, mesh.shape["tm"], mesh.shape["rows"]),
        mesh=mesh,
        in_specs=(
            P("tm", "rows", None, None), P(), P(), P(), P("tm", None, "rows", None), P(), P(), P(),
        ),
        out_specs=P("tm", "rows", None, None),
        check_vma=False,
    )
```

```python
import functools

import jax
import jax.numpy as jnp
from jax import lax
from jax.experimental import pallas as pl
from jax.experimental.pallas import tpu as pltpu
from jax.sharding import PartitionSpec as P

epsilon = 1e-06
haar_scale = 0.35355339059327373
MESH = pl.DeviceIdType.MESH
BF = jnp.bfloat16
F32 = jnp.float32


def norm_silu(x, half_gain):
    mean = jnp.mean(x, axis=-1, keepdims=True)
    c = x - mean
    var = jnp.mean(c * c, axis=-1, keepdims=True)
    h = c * lax.rsqrt(var + epsilon) * half_gain
    return (h + h * jnp.tanh(h)).astype(BF)


def shift_down(x):
    row = lax.broadcasted_iota(jnp.int32, x.shape, 0)
    return jnp.where(row == 0, 0.0, pltpu.roll(x, 1, 0))


def shift_up(x):
    n = x.shape[0]
    row = lax.broadcasted_iota(jnp.int32, x.shape, 0)
    return jnp.where(row == n - 1, 0.0, pltpu.roll(x, n - 1, 0))


def kernel(
    n_tm, n_rows,
    feat, gain_mid, conv_mid, down, wav, inj, gain_deep, conv_deep,
    out,
    fv, wm, wdn, wd, wv, iv, injw, wavt, xp, xv, um, ym, pe, lv, sb, fd, yp, yd,
    lsem, send, recv,
    *accs,
):
    t_id, r_id = lax.axis_index("tm"), lax.axis_index("rows")
    has_prev, has_next = t_id > 0, t_id < n_tm - 1
    has_up, has_dn = r_id > 0, r_id < n_rows - 1
    acc = (accs[:8], accs[8:])

    def load(i, src, dst):
        return pltpu.make_async_copy(src, dst, lsem.at[i])

    feat_loads = [load(i, feat.at[i], fv.at[i]) for i in range(4)]
    for i in (3, 2, 1, 0):
        feat_loads[i].start()
    ld_wm = load(4, conv_mid, wm)
    ld_dn = load(5, down, wdn)
    ld_wv = load(6, wav, wv)
    ld_iv = load(7, inj, iv)
    ld_wd = load(8, conv_deep, wd)
    for ld in (ld_wm, ld_wv, ld_iv, ld_dn, ld_wd):
        ld.start()

    barrier = pltpu.get_barrier_semaphore()
    count = jnp.int32(0)
    for dt in (-1, 0, 1):
        for dr in (-1, 0, 1):
            if dt == 0 and dr == 0:
                continue
            there = jnp.bool_(True)
            if dt:
                there = has_prev if dt < 0 else has_next
            if dr:
                there_r = has_up if dr < 0 else has_dn
                there = jnp.logical_and(there, there_r) if dt else there_r
            count = count + there.astype(jnp.int32)

            @pl.when(there)
            def _():
                pl.semaphore_signal(
                    barrier, inc=1, device_id=(t_id + dt, r_id + dr), device_id_type=MESH
                )

    halo = {}

    def both(dt, dr):
        cond = {-1: (has_prev, has_up), 1: (has_next, has_dn)}
        target, source = None, None
        if dt:
            target, source = cond[dt][0], cond[-dt][0]
        if dr:
            tr, sr = cond[dr][1], cond[-dr][1]
            target = tr if target is None else jnp.logical_and(target, tr)
            source = sr if source is None else jnp.logical_and(source, sr)
        return target, source

    def add_halo(name, src, dst, dt, dr, only=None):
        i = len(halo)
        desc = pltpu.make_async_remote_copy(
            src_ref=src, dst_ref=dst, send_sem=send.at[i], recv_sem=recv.at[i],
            device_id=(t_id + dt, r_id + dr), device_id_type=MESH,
        )
        target, source = both(dt, dr)
        if only is not None:
            target, source = jnp.logical_and(target, only), jnp.logical_and(source, only)
        halo[name] = (desc, target, source)

    add_halo("u", xp.at[2:6, 1], xp.at[2:6, 9], 0, -1)
    add_halo("d", xp.at[2:6, 8], xp.at[2:6, 0], 0, 1)
    add_halo("ze1", xp.at[4:6, 1], xp.at[0:2, 1], 1, 0)
    add_halo("ze8", xp.at[4:6, 8], xp.at[0:2, 8], 1, 0)
    add_halo("z3", xp.at[5, 2:8], xp.at[1, 2:8], 1, 0)
    add_halo("z2", xp.at[4, 2:8], xp.at[0, 2:8], 1, 0)
    add_halo("cu", xp.at[0:2, 1], xp.at[0:2, 9], 0, -1, has_prev)
    add_halo("cd", xp.at[0:2, 8], xp.at[0:2, 0], 0, 1, has_prev)
    for f in (1, 0):
        add_halo(f"yu{f}", yp.at[2 + f, 1], yp.at[2 + f, 5], 0, -1)
        add_halo(f"yd{f}", yp.at[2 + f, 4], yp.at[2 + f, 0], 0, 1)
        add_halo(f"yz{f}", yp.at[2 + f, 1:5], yp.at[f, 1:5], 1, 0)
        add_halo(f"yzu{f}", yp.at[2 + f, 1], yp.at[f, 5], 1, -1)
        add_halo(f"yzd{f}", yp.at[2 + f, 4], yp.at[f, 0], 1, 1)

    def start(*names):
        for name in names:
            desc, target, _ = halo[name]
            pl.when(target)(desc.start)

    def arrive(*names):
        for name in names:
            desc, _, source = halo[name]
            pl.when(source)(desc.wait_recv)

    @pl.when(jnp.logical_not(has_prev))
    def _():
        xp[0:2] = jnp.zeros((2, 10, 128, 256), BF)
        yp[0:2] = jnp.zeros((2, 6, 64, 512), BF)

    @pl.when(jnp.logical_not(has_up))
    def _():
        xp[:, 0] = jnp.zeros((6, 128, 256), BF)
        yp[:, 0] = jnp.zeros((4, 64, 512), BF)

    @pl.when(jnp.logical_not(has_dn))
    def _():
        xp[:, 9] = jnp.zeros((6, 128, 256), BF)
        yp[:, 5] = jnp.zeros((4, 64, 512), BF)

    half_gain = gain_mid[...] * 0.5

    def norm_row(f, r):
        for piece in range(2):
            rows = pl.ds(piece * 64, 64)
            xp[f + 2, r + 1, rows, :] = norm_silu(fv[f, r, rows, :].astype(F32), half_gain)

    for f in (3, 2, 1, 0):
        feat_loads[f].wait()

    @pl.loop(0, 4)
    def _(f):
        norm_row(f, 0)
        norm_row(f, 7)

    pl.semaphore_wait(barrier, count)
    start("u", "d", "ze1", "ze8")
    for f in (3, 2, 1):
        @pl.loop(0, 3)
        def _(r):
            norm_row(f, 2 * r + 1)
            norm_row(f, 2 * r + 2)

        if f == 3:
            start("z3")
        if f == 2:
            start("z2")

    injw[...] = jnp.zeros((256, 512), BF)
    wavt[...] = jnp.zeros((2, 256, 256), BF)
    ld_wv.wait()
    ld_iv.wait()
    injw[0:24, :] = iv[...]
    for t in range(2):
        coeffs = wv[t].astype(F32)
        for h in range(4):
            wavt[t, h * 64:(h + 1) * 64, 0:24] = coeffs[:, h, :].T.astype(BF)

    bands = ((1, 2), (0, 3))

    def weight_rows(a, c):
        for piece in range(4):
            rows = pl.ds(piece * 64, 64)
            g = [wm[(a * 3 + b) * 3 + c, rows, :].astype(F32) for b in range(3)]
            side = g[0] + g[2]
            um[a, c, 0, rows, :] = ((side + g[1]) * 0.5).astype(BF)
            um[a, c, 1, rows, :] = ((side - g[1]) * 0.5).astype(BF)

    def data_rows(f, p):
        for piece in range(4):
            rows = pl.ds(piece * 32, 32)
            d = [xp[f, 2 * p + j, rows, :] for j in range(4)]
            xv[f, p, 0, rows, :] = d[0] - d[2]
            xv[f, p, 1, rows, :] = d[1] + d[2]
            xv[f, p, 2, rows, :] = d[2] - d[1]
            xv[f, p, 3, rows, :] = d[1] - d[3]

    def data_band(f, band):
        for p in bands[band]:
            data_rows(f, p)

    def mid_weight(i, a, c):
        if i == 0:
            return wm[a * 9 + c]
        if i == 3:
            return wm[a * 9 + 6 + c]
        return um[a, c, i - 1]

    def mid_block(t, band, depths, slot):
        for c in range(3):
            base = 4 * (c % 2)
            k = 0
            for e in range(2):
                for a in depths:
                    for q in range(2):
                        i = 2 * q + e
                        pltpu.matmul_push_rhs(mid_weight(i, a, c), k % 2, q)
                        for h in range(2):
                            pltpu.matmul_acc_lhs(
                                acc[q][base + e * 2 + h], xv[t + a, bands[band][h], i],
                                load_staged_rhs=k % 2 if h == 0 else None,
                            )
                    k += 1
                for q in range(2):
                    for h in range(2):
                        ym[slot, h, c, 2 * q + e] = pltpu.matmul_pop(acc[q][base + e * 2 + h])

    def mid_combine(t, band, slot, early=False, late=False):
        for h in range(2):
            p = bands[band][h]
            for n in range(2):
                lanes = pl.ds(n * 128, 128)
                pair = ([], [])
                for c in range(3):
                    m = [ym[slot, h, c, i, :, lanes] for i in range(4)]
                    pair[0].append(m[0] + (m[1] + m[2]))
                    pair[1].append((m[1] - m[2]) - m[3])
                for j in range(2):
                    r = 2 * p + j
                    total = shift_down(pair[j][0]) + pair[j][1] + shift_up(pair[j][2])
                    if late:
                        total = total + pe[t, r, :, lanes]
                    if early:
                        pe[t, r, :, lanes] = total
                    else:
                        level = (fv[t, r, :, lanes].astype(F32) + total).astype(BF)
                        lv[t % 2, n, r] = level.astype(F32)

    def mid_full(t, band, slot):
        mid_block(t, band, (0, 1, 2), slot)
        mid_combine(t, band, slot)

    def mid_early(t, band, slot):
        mid_block(t, band, (2, 1) if t == 1 else (2,), slot)
        mid_combine(t, band, slot, early=True)

    def mid_late(t, band, slot):
        mid_block(t, band, (0,) if t == 1 else (1, 0), slot)
        mid_combine(t, band, slot, late=True)

    half_gain_deep = gain_deep[...] * 0.5

    def deep_frame(t):
        @pl.loop(0, 4)
        def _(r):
            for piece in range(4):
                for n in range(2):
                    lanes = pl.ds(n * 128, 128)
                    v = {}
                    for i in range(2):
                        for j in range(2):
                            for k in range(2):
                                v[i, j, k] = lv[
                                    i, n, 2 * r + j, pl.ds(piece * 32 + k, 16, stride=2), :
                                ]
                    for axis in range(3):
                        w = {}
                        for key in v:
                            if key[axis] == 0:
                                other = key[:axis] + (1,) + key[axis + 1:]
                                w[key] = v[key] + v[other]
                                w[other] = v[key] - v[other]
                        v = w
                    for i in range(2):
                        for j in range(2):
                            for k in range(2):
                                s = 4 * i + 2 * j + k
                                row = pl.multiple_of(r * 64 + piece * 16, 16)
                                sb[s, pl.ds(row, 16), lanes] = (v[i, j, k] * haar_scale).astype(BF)

        for s in range(9):
            for q in range(2):
                cols = slice(q * 256, (q + 1) * 256)
                rhs = wdn[s, :, cols] if s < 8 else injw[:, cols]
                pltpu.matmul_push_rhs(rhs, s % 2, q)
                for h in range(2):
                    rows = slice(h * 128, (h + 1) * 128)
                    lhs = sb[s, rows, :] if s < 8 else wavt[t, rows, :]
                    pltpu.matmul_acc_lhs(acc[q][h], lhs, load_staged_rhs=s % 2 if h == 0 else None)
        for h in range(2):
            for q in range(2):
                fd[t, h * 128:(h + 1) * 128, q * 256:(q + 1) * 256] = pltpu.matmul_pop(acc[q][h])

        @pl.loop(0, 4)
        def _(r):
            for piece in range(2):
                rows = pl.ds(pl.multiple_of(r * 64 + piece * 32, 32), 32)
                yp[t + 2, r + 1, pl.ds(piece * 32, 32), :] = norm_silu(fd[t, rows, :], half_gain_deep)

    def start_deep(f):
        start(f"yu{f}", f"yd{f}", f"yz{f}", f"yzu{f}", f"yzd{f}")

    ld_wm.wait()
    for c in range(3):
        for a in range(3):
            weight_rows(a, c)
    for f in (3, 4, 5):
        data_band(f, 0)
    mid_full(3, 0, 0)
    for r in range(1, 7):
        norm_row(0, r)
    data_band(2, 0)
    mid_full(2, 0, 1)
    arrive("ze1", "ze8")
    start("cu", "cd")
    mid_early(1, 0, 0)
    mid_early(0, 0, 1)
    arrive("u", "d")
    for f in (3, 4, 5, 2):
        data_band(f, 1)
    mid_full(3, 1, 0)
    mid_full(2, 1, 1)
    ld_dn.wait()
    deep_frame(1)
    start_deep(1)
    mid_early(1, 1, 0)
    mid_early(0, 1, 1)
    arrive("z3", "cu", "cd")
    data_band(1, 0)
    data_band(1, 1)
    mid_late(1, 0, 0)
    mid_late(1, 1, 1)
    arrive("z2")
    data_band(0, 0)
    data_band(0, 1)
    mid_late(0, 0, 0)
    mid_late(0, 1, 1)
    deep_frame(0)
    start_deep(0)

    ld_wd.wait()

    def deep_conv(t, order, base=None):
        k = 0
        for step, (a, names) in enumerate(order):
            arrive(*names)
            for c in range(3):
                for b in range(3):
                    tap = (a * 3 + b) * 3 + c
                    for d in range(2):
                        depth = slice(d * 256, (d + 1) * 256)
                        for q in range(2):
                            pltpu.matmul_push_rhs(
                                wd[tap, depth, q * 256:(q + 1) * 256], k % 2, q
                            )
                            for h in range(2):
                                lhs = yp[t + a, b + 2 * h:b + 2 * h + 2, :, depth]
                                pltpu.matmul_acc_lhs(
                                    acc[q][c * 2 + h], lhs.reshape(128, 256),
                                    load_staged_rhs=k % 2 if h == 0 else None,
                                )
                        k += 1
                if step == len(order) - 1:
                    for q in range(2):
                        for h in range(2):
                            block = (c, slice(h * 128, (h + 1) * 128), slice(q * 256, (q + 1) * 256))
                            total = pltpu.matmul_pop(acc[q][c * 2 + h])
                            if base is not None:
                                total = total + base[block]
                            yd[(t,) + block] = total

    def deep_combine(t):
        for r in range(4):
            rows = slice(r * 64, (r + 1) * 64)
            for n in range(4):
                lanes = slice(n * 128, (n + 1) * 128)
                total = shift_down(yd[t, 0, rows, lanes]) + yd[t, 1, rows, lanes]
                total = total + shift_up(yd[t, 2, rows, lanes])
                out[t, r, :, lanes] = (fd[t, rows, lanes] + total).astype(BF)

    arrive("yu1", "yd1", "yz1", "yzu1", "yzd1")
    deep_conv(0, ((1, ()),))
    deep_conv(1, ((2, ()), (0, ()), (1, ("yu0", "yd0"))))
    deep_combine(1)
    deep_conv(0, ((2, ()), (0, ("yz0", "yzu0", "yzd0"))), yd.at[0])
    deep_combine(0)

    for desc, target, _ in halo.values():
        pl.when(target)(desc.wait_send)


def on_device(n_tm, n_rows, feat, gain_mid, conv_mid, down, wav, inj, gain_deep, conv_deep):
    def body(*refs):
        def inner(*accs):
            kernel(n_tm, n_rows, *refs, *accs)

        pl.run_scoped(inner, *[pltpu.ACC(q)((128, 256), F32) for q in range(2) for _ in range(8)])

    hbm = pl.BlockSpec(memory_space=pltpu.HBM)
    vmem = pl.BlockSpec(memory_space=pltpu.VMEM)
    return pl.pallas_call(
        body,
        out_shape=pltpu.VMEM((2, 4, 64, 512), BF),
        in_specs=[hbm, vmem, hbm, hbm, hbm, hbm, vmem, hbm],
        out_specs=vmem,
        scratch_shapes=[
            pltpu.VMEM((4, 8, 128, 256), BF),
            pltpu.VMEM((27, 256, 256), BF),
            pltpu.VMEM((8, 256, 512), BF),
            pltpu.VMEM((27, 512, 512), BF),
            pltpu.VMEM((2, 24, 4, 64), BF),
            pltpu.VMEM((24, 512), BF),
            pltpu.VMEM((256, 512), BF),
            pltpu.VMEM((2, 256, 256), BF),
            pltpu.VMEM((6, 10, 128, 256), BF),
            pltpu.VMEM((6, 4, 4, 128, 256), BF),
            pltpu.VMEM((3, 3, 2, 256, 256), BF),
            pltpu.VMEM((2, 2, 3, 4, 128, 256), F32),
            pltpu.VMEM((2, 8, 128, 256), F32),
            pltpu.VMEM((2, 2, 8, 128, 128), F32),
            pltpu.VMEM((8, 256, 256), BF),
            pltpu.VMEM((2, 256, 512), F32),
            pltpu.VMEM((4, 6, 64, 512), BF),
            pltpu.VMEM((2, 3, 256, 512), F32),
            pltpu.SemaphoreType.DMA((9,)),
            pltpu.SemaphoreType.DMA((18,)),
            pltpu.SemaphoreType.DMA((18,)),
        ],
        compiler_params=pltpu.CompilerParams(
            collective_id=0, has_side_effects=True, vmem_limit_bytes=60 * 1000 * 1000
        ),
    )(*[
        pltpu.with_memory_space_constraint(x, pltpu.HBM)
        for x in (
            feat, gain_mid.reshape(1, 256), conv_mid.reshape(27, 256, 256), down, wav, inj,
            gain_deep.reshape(1, 512), conv_deep.reshape(27, 512, 512),
        )
    ])


def solution(mesh):
    return jax.shard_map(
        functools.partial(on_device, mesh.shape["tm"], mesh.shape["rows"]),
        mesh=mesh,
        in_specs=(
            P("tm", "rows", None, None), P(), P(), P(), P("tm", None, "rows", None), P(), P(), P(),
        ),
        out_specs=P("tm", "rows", None, None),
        check_vma=False,
    )
```

```python
import functools

import jax
import jax.numpy as jnp
from jax import lax
from jax.experimental import pallas as pl
from jax.experimental.pallas import tpu as pltpu
from jax.sharding import PartitionSpec as P

epsilon = 1e-06
haar_scale = 0.35355339059327373
MESH = pl.DeviceIdType.MESH
BF = jnp.bfloat16
F32 = jnp.float32


def norm_silu(x, half_gain):
    mean = jnp.mean(x, axis=-1, keepdims=True)
    c = x - mean
    var = jnp.mean(c * c, axis=-1, keepdims=True)
    h = c * lax.rsqrt(var + epsilon) * half_gain
    return (h + h * jnp.tanh(h)).astype(BF)


def shift_down(x):
    moved = pltpu.roll(x, 1, 0)
    row = lax.broadcasted_iota(jnp.int32, (8, x.shape[1]), 0)
    return jnp.concatenate([jnp.where(row == 0, 0.0, moved[:8]), moved[8:]], axis=0)


def shift_up(x):
    n = x.shape[0]
    moved = pltpu.roll(x, n - 1, 0)
    row = lax.broadcasted_iota(jnp.int32, (8, x.shape[1]), 0)
    return jnp.concatenate([moved[:n - 8], jnp.where(row == 7, 0.0, moved[n - 8:])], axis=0)


def kernel(
    n_tm, n_rows,
    feat, gain_mid, conv_mid, down, wav, inj, gain_deep, conv_deep,
    out,
    fv, wm, wdn, wd, wv, iv, injw, wavt, xp, xv, um, ym0, ym1, pe, ff, lv, sb, fd, yp, yd0, yd1,
    lsem, send, recv,
    *accs,
):
    t_id, r_id = lax.axis_index("tm"), lax.axis_index("rows")
    has_prev, has_next = t_id > 0, t_id < n_tm - 1
    has_up, has_dn = r_id > 0, r_id < n_rows - 1
    acc = (accs[:8], accs[8:])
    ym = (ym0, ym1)
    yd = (yd0, yd1)

    def load(i, src, dst):
        return pltpu.make_async_copy(src, dst, lsem.at[i])

    feat_loads = [load(i, feat.at[i], fv.at[i]) for i in range(4)]
    for i in (3, 2, 1, 0):
        feat_loads[i].start()
    ld_wm = load(4, conv_mid, wm)
    ld_dn = load(5, down, wdn)
    ld_wv = load(6, wav, wv)
    ld_iv = load(7, inj, iv)
    ld_wd = load(8, conv_deep, wd)
    for ld in (ld_wm, ld_wv, ld_iv, ld_dn, ld_wd):
        ld.start()

    barrier = pltpu.get_barrier_semaphore()
    count = jnp.int32(0)
    for dt in (-1, 0, 1):
        for dr in (-1, 0, 1):
            if dt == 0 and dr == 0:
                continue
            there = jnp.bool_(True)
            if dt:
                there = has_prev if dt < 0 else has_next
            if dr:
                there_r = has_up if dr < 0 else has_dn
                there = jnp.logical_and(there, there_r) if dt else there_r
            count = count + there.astype(jnp.int32)

            @pl.when(there)
            def _():
                pl.semaphore_signal(
                    barrier, inc=1, device_id=(t_id + dt, r_id + dr), device_id_type=MESH
                )

    halo = {}

    def both(dt, dr):
        cond = {-1: (has_prev, has_up), 1: (has_next, has_dn)}
        target, source = None, None
        if dt:
            target, source = cond[dt][0], cond[-dt][0]
        if dr:
            tr, sr = cond[dr][1], cond[-dr][1]
            target = tr if target is None else jnp.logical_and(target, tr)
            source = sr if source is None else jnp.logical_and(source, sr)
        return target, source

    def add_halo(name, src, dst, dt, dr, only=None):
        i = len(halo)
        desc = pltpu.make_async_remote_copy(
            src_ref=src, dst_ref=dst, send_sem=send.at[i], recv_sem=recv.at[i],
            device_id=(t_id + dt, r_id + dr), device_id_type=MESH,
        )
        target, source = both(dt, dr)
        if only is not None:
            target, source = jnp.logical_and(target, only), jnp.logical_and(source, only)
        halo[name] = (desc, target, source)

    add_halo("u", xp.at[3:6, 1], xp.at[3:6, 9], 0, -1)
    add_halo("d", xp.at[3:6, 8], xp.at[3:6, 0], 0, 1)
    add_halo("u0", xp.at[2, 1], xp.at[2, 9], 0, -1)
    add_halo("d0", xp.at[2, 8], xp.at[2, 0], 0, 1)
    add_halo("ze1", xp.at[4:6, 1], xp.at[0:2, 1], 1, 0)
    add_halo("ze8", xp.at[4:6, 8], xp.at[0:2, 8], 1, 0)
    add_halo("z3", xp.at[5, 2:8], xp.at[1, 2:8], 1, 0)
    add_halo("z2", xp.at[4, 2:8], xp.at[0, 2:8], 1, 0)
    add_halo("cu", xp.at[0:2, 1], xp.at[0:2, 9], 0, -1, has_prev)
    add_halo("cd", xp.at[0:2, 8], xp.at[0:2, 0], 0, 1, has_prev)
    for f in (1, 0):
        add_halo(f"yu{f}", yp.at[2 + f, 1], yp.at[2 + f, 5], 0, -1)
        add_halo(f"yd{f}", yp.at[2 + f, 4], yp.at[2 + f, 0], 0, 1)
        add_halo(f"yz{f}", yp.at[2 + f, 1:5], yp.at[f, 1:5], 1, 0)
        add_halo(f"yzu{f}", yp.at[2 + f, 1], yp.at[f, 5], 1, -1)
        add_halo(f"yzd{f}", yp.at[2 + f, 4], yp.at[f, 0], 1, 1)

    def start(*names):
        for name in names:
            desc, target, _ = halo[name]
            pl.when(target)(desc.start)

    def arrive(*names):
        for name in names:
            desc, _, source = halo[name]
            pl.when(source)(desc.wait_recv)

    @pl.when(jnp.logical_not(has_prev))
    def _():
        xp[0:2] = jnp.zeros((2, 10, 128, 256), BF)
        yp[0:2] = jnp.zeros((2, 6, 64, 512), BF)

    @pl.when(jnp.logical_not(has_up))
    def _():
        xp[:, 0] = jnp.zeros((6, 128, 256), BF)
        yp[:, 0] = jnp.zeros((4, 64, 512), BF)

    @pl.when(jnp.logical_not(has_dn))
    def _():
        xp[:, 9] = jnp.zeros((6, 128, 256), BF)
        yp[:, 5] = jnp.zeros((4, 64, 512), BF)

    for slot in range(2):
        for end in (0, 136):
            ym[slot][:, :, :, :, end:end + 8, :] = jnp.zeros((2, 3, 4, 2, 8, 128), F32)

    half_gain = gain_mid[...] * 0.5

    def norm_row(f, r):
        for piece in range(2):
            rows = pl.ds(piece * 64, 64)
            x = fv[f, r, rows, :].astype(F32)
            xp[f + 2, r + 1, rows, :] = norm_silu(x, half_gain)
            for n in range(2):
                ff[f, r, n, rows, :] = x[:, n * 128:(n + 1) * 128]

    for f in (3, 2, 1, 0):
        feat_loads[f].wait()

    @pl.loop(0, 4)
    def _(f):
        norm_row(f, 0)
        norm_row(f, 7)

    pl.semaphore_wait(barrier, count)
    start("u", "d", "ze1", "ze8", "u0", "d0")
    for f in (3, 2, 1):
        @pl.loop(0, 3)
        def _(r):
            norm_row(f, 2 * r + 1)
            norm_row(f, 2 * r + 2)

        if f == 3:
            start("z3")
        if f == 2:
            start("z2")

    injw[...] = jnp.zeros((256, 512), BF)
    wavt[...] = jnp.zeros((2, 256, 256), BF)
    ld_wv.wait()
    ld_iv.wait()
    injw[0:24, :] = iv[...]
    for t in range(2):
        coeffs = wv[t].astype(F32)
        for h in range(4):
            wavt[t, h * 64:(h + 1) * 64, 0:24] = coeffs[:, h, :].T.astype(BF)

    bands = ((1, 2), (0, 3))

    def weight_rows(a, c):
        for piece in range(4):
            rows = pl.ds(piece * 64, 64)
            g = [wm[(a * 3 + b) * 3 + c, rows, :] for b in range(3)]
            side = g[0] + g[2]
            um[a, c, 0, rows, :] = (side + g[1]) * jnp.bfloat16(0.5)
            um[a, c, 1, rows, :] = (side - g[1]) * jnp.bfloat16(0.5)

    def data_rows(f, p):
        for piece in range(4):
            rows = pl.ds(piece * 32, 32)
            d = [xp[f, 2 * p + j, rows, :] for j in range(4)]
            xv[f, p, 0, rows, :] = d[0] - d[2]
            xv[f, p, 1, rows, :] = d[1] + d[2]
            xv[f, p, 2, rows, :] = d[2] - d[1]
            xv[f, p, 3, rows, :] = d[1] - d[3]

    def data_band(f, band):
        for p in bands[band]:
            data_rows(f, p)

    def mid_weight(i, a, c):
        if i == 0:
            return wm[a * 9 + c]
        if i == 3:
            return wm[a * 9 + 6 + c]
        return um[a, c, i - 1]

    def mid_block(t, band, depths, slot):
        for c in range(3):
            base = 4 * (c % 2)
            k = 0
            for e in range(2):
                for a in depths:
                    for q in range(2):
                        i = 2 * q + e
                        pltpu.matmul_push_rhs(mid_weight(i, a, c), k % 2, q)
                        for h in range(2):
                            pltpu.matmul_acc_lhs(
                                acc[q][base + e * 2 + h], xv[t + a, bands[band][h], i],
                                load_staged_rhs=k % 2 if h == 0 else None,
                            )
                    k += 1
                for q in range(2):
                    for h in range(2):
                        product = pltpu.matmul_pop(acc[q][base + e * 2 + h])
                        for n in range(2):
                            ym[slot][h, c, 2 * q + e, n, 8:136, :] = product[:, n * 128:(n + 1) * 128]

    def mid_combine(t, band, slot, early=False, late=False):
        for h in range(2):
            p = bands[band][h]
            for n in range(2):
                for odd in range(2):
                    for piece in range(4):
                        z = []
                        for i in range(4):
                            terms = [
                                ym[slot][h, c, i, n, pl.ds(7 + c + odd + 32 * piece, 16, stride=2), :]
                                for c in range(3)
                            ]
                            z.append(terms[0] + terms[1] + terms[2])
                        pair = (z[0] + (z[1] + z[2]), (z[1] - z[2]) - z[3])
                        place = pl.ds(16 * piece, 16)
                        for j in range(2):
                            r = 2 * p + j
                            total = pair[j]
                            if late:
                                total = total + pe[t, n, r, odd, place, :]
                            else:
                                total = total + ff[t, r, n, pl.ds(odd + 32 * piece, 16, stride=2), :]
                            if early:
                                pe[t, n, r, odd, place, :] = total
                            else:
                                lv[t % 2, n, r, odd, place, :] = total.astype(BF).astype(F32)

    pending = []

    def flush():
        while pending:
            pending.pop(0)()

    def mid_step(t, band, depths, **kind):
        slot = mid_step.count % 2
        mid_step.count += 1
        mid_block(t, band, depths, slot)
        flush()
        pending.append(lambda: mid_combine(t, band, slot, **kind))

    mid_step.count = 0

    def mid_full(t, band):
        mid_step(t, band, (0, 1, 2))

    def mid_early(t, band):
        mid_step(t, band, (2, 1) if t == 1 else (2,), early=True)

    def mid_late(t, band):
        mid_step(t, band, (0,) if t == 1 else (1, 0), late=True)

    half_gain_deep = gain_deep[...] * 0.5

    def haar(t):
        for r in range(4):
            for piece in range(4):
                for n in range(2):
                    lanes = pl.ds(n * 128, 128)
                    v = {}
                    for i in range(2):
                        for j in range(2):
                            for k in range(2):
                                v[i, j, k] = lv[
                                    i, n, 2 * r + j, k, pl.ds(piece * 16, 16), :
                                ]
                    for axis in range(3):
                        w = {}
                        for key in v:
                            if key[axis] == 0:
                                other = key[:axis] + (1,) + key[axis + 1:]
                                w[key] = v[key] + v[other]
                                w[other] = v[key] - v[other]
                        v = w
                    for i in range(2):
                        for j in range(2):
                            for k in range(2):
                                s = 4 * i + 2 * j + k
                                row = r * 64 + piece * 16
                                sb[s, pl.ds(row, 16), lanes] = (v[i, j, k] * haar_scale).astype(BF)

    def project(t):
        for s in range(9):
            for q in range(2):
                cols = slice(q * 256, (q + 1) * 256)
                rhs = wdn[s, :, cols] if s < 8 else injw[:, cols]
                pltpu.matmul_push_rhs(rhs, s % 2, q)
                for h in range(2):
                    rows = slice(h * 128, (h + 1) * 128)
                    lhs = sb[s, rows, :] if s < 8 else wavt[t, rows, :]
                    pltpu.matmul_acc_lhs(acc[q][h], lhs, load_staged_rhs=s % 2 if h == 0 else None)
        for h in range(2):
            for q in range(2):
                fd[t, h * 128:(h + 1) * 128, q * 256:(q + 1) * 256] = pltpu.matmul_pop(acc[q][h])

    def deep_norm(t):
        for r in range(4):
            for piece in range(2):
                rows = pl.ds(r * 64 + piece * 32, 32)
                yp[t + 2, r + 1, pl.ds(piece * 32, 32), :] = norm_silu(fd[t, rows, :], half_gain_deep)

    def start_deep(f):
        start(f"yu{f}", f"yd{f}", f"yz{f}", f"yzu{f}", f"yzd{f}")

    ld_wm.wait()
    for c in range(3):
        for a in range(3):
            weight_rows(a, c)
    for f in (3, 4, 5):
        data_band(f, 0)
    def deep_conv(t, order, base=None):
        k = 0
        for step, (a, names) in enumerate(order):
            arrive(*names)
            for c in range(3):
                for b in range(3):
                    tap = (a * 3 + b) * 3 + c
                    for d in range(2):
                        depth = slice(d * 256, (d + 1) * 256)
                        for q in range(2):
                            pltpu.matmul_push_rhs(
                                wd[tap, depth, q * 256:(q + 1) * 256], k % 2, q
                            )
                            for h in range(2):
                                lhs = yp[t + a, b + 2 * h:b + 2 * h + 2, :, depth]
                                pltpu.matmul_acc_lhs(
                                    acc[q][c * 2 + h], lhs.reshape(128, 256),
                                    load_staged_rhs=k % 2 if h == 0 else None,
                                )
                        k += 1
                if step == len(order) - 1:
                    for q in range(2):
                        for h in range(2):
                            block = (c, slice(h * 128, (h + 1) * 128), slice(q * 256, (q + 1) * 256))
                            total = pltpu.matmul_pop(acc[q][c * 2 + h])
                            if base is not None:
                                total = total + base[block]
                            yd[t][block] = total

    def deep_combine(t):
        for r in range(4):
            rows = slice(r * 64, (r + 1) * 64)
            for n in range(4):
                lanes = slice(n * 128, (n + 1) * 128)
                total = shift_down(yd[t][0, rows, lanes]) + yd[t][1, rows, lanes]
                total = total + shift_up(yd[t][2, rows, lanes])
                out[t, r, :, lanes] = (fd[t, rows, lanes] + total).astype(BF)

    mid_full(3, 0)
    for r in range(1, 7):
        norm_row(0, r)
    data_band(2, 0)
    mid_full(2, 0)
    arrive("ze1", "ze8")
    start("cu", "cd")
    mid_early(1, 0)
    mid_early(0, 0)
    arrive("u", "d")
    for f in (3, 4, 5):
        data_band(f, 1)
    mid_full(3, 1)
    arrive("u0", "d0")
    data_band(2, 1)
    mid_full(2, 1)
    mid_early(1, 1)
    ld_dn.wait()
    haar(1)
    project(1)
    deep_norm(1)
    start_deep(1)
    mid_early(0, 1)
    arrive("z3", "cu", "cd")
    data_band(1, 0)
    data_band(1, 1)
    mid_late(1, 0)
    mid_late(1, 1)
    arrive("z2")
    data_band(0, 0)
    data_band(0, 1)
    mid_late(0, 0)
    mid_late(0, 1)
    flush()
    haar(0)
    project(0)
    deep_norm(0)
    start_deep(0)
    ld_wd.wait()
    arrive("yu1", "yd1", "yz1", "yzu1", "yzd1")
    deep_conv(0, ((1, ()),))
    deep_conv(1, ((2, ()), (0, ()), (1, ("yu0", "yd0"))))
    deep_combine(1)
    deep_conv(0, ((2, ()), (0, ("yz0", "yzu0", "yzd0"))), yd0)
    deep_combine(0)

    for desc, target, _ in halo.values():
        pl.when(target)(desc.wait_send)


def on_device(n_tm, n_rows, feat, gain_mid, conv_mid, down, wav, inj, gain_deep, conv_deep):
    def body(*refs):
        def inner(*accs):
            kernel(n_tm, n_rows, *refs, *accs)

        pl.run_scoped(inner, *[pltpu.ACC(q)((128, 256), F32) for q in range(2) for _ in range(8)])

    hbm = pl.BlockSpec(memory_space=pltpu.HBM)
    vmem = pl.BlockSpec(memory_space=pltpu.VMEM)
    return pl.pallas_call(
        body,
        out_shape=pltpu.VMEM((2, 4, 64, 512), BF),
        in_specs=[hbm, vmem, hbm, hbm, hbm, hbm, vmem, hbm],
        out_specs=vmem,
        scratch_shapes=[
            pltpu.VMEM((4, 8, 128, 256), BF),
            pltpu.VMEM((27, 256, 256), BF),
            pltpu.VMEM((8, 256, 512), BF),
            pltpu.VMEM((27, 512, 512), BF),
            pltpu.VMEM((2, 24, 4, 64), BF),
            pltpu.VMEM((24, 512), BF),
            pltpu.VMEM((256, 512), BF),
            pltpu.VMEM((2, 256, 256), BF),
            pltpu.VMEM((6, 10, 128, 256), BF),
            pltpu.VMEM((6, 4, 4, 128, 256), BF),
            pltpu.VMEM((3, 3, 2, 256, 256), BF),
            pltpu.VMEM((2, 3, 4, 2, 144, 128), F32),
            pltpu.VMEM((2, 3, 4, 2, 144, 128), F32),
            pltpu.VMEM((2, 2, 8, 2, 64, 128), F32),
            pltpu.VMEM((4, 8, 2, 128, 128), F32),
            pltpu.VMEM((2, 2, 8, 2, 64, 128), F32),
            pltpu.VMEM((8, 256, 256), BF),
            pltpu.VMEM((2, 256, 512), F32),
            pltpu.VMEM((4, 6, 64, 512), BF),
            pltpu.VMEM((3, 256, 512), F32),
            pltpu.VMEM((3, 256, 512), F32),
            pltpu.SemaphoreType.DMA((9,)),
            pltpu.SemaphoreType.DMA((20,)),
            pltpu.SemaphoreType.DMA((20,)),
        ],
        compiler_params=pltpu.CompilerParams(
            collective_id=0, has_side_effects=True, vmem_limit_bytes=63 * 1000 * 1000
        ),
    )(*[
        pltpu.with_memory_space_constraint(x, pltpu.HBM)
        for x in (
            feat, gain_mid.reshape(1, 256), conv_mid.reshape(27, 256, 256), down, wav, inj,
            gain_deep.reshape(1, 512), conv_deep.reshape(27, 512, 512),
        )
    ])


def solution(mesh):
    return jax.shard_map(
        functools.partial(on_device, mesh.shape["tm"], mesh.shape["rows"]),
        mesh=mesh,
        in_specs=(
            P("tm", "rows", None, None), P(), P(), P(), P("tm", None, "rows", None), P(), P(), P(),
        ),
        out_specs=P("tm", "rows", None, None),
        check_vma=False,
    )
```
